32 devices in a mesh: ep: 8 (over y, x, core), dp: 4 (over z).
Axes of the slice: x: 2, y: 2, z: 4, core: 2. Of those that a mesh axis runs over, the one named last changes fastest.
Arguments:
- master_weights: float32 [8, 1024, 3584], P('ep', 'dp'), may hold values from -6 to 6
- first_moment: float32 [8, 1024, 3584], P('ep', 'dp'), may hold values from -6 to 6
- second_moment: float32 [8, 1024, 3584], P('ep', 'dp'), may hold values from 0.01 to 4
- expert_ids: int32 [8], replicated, may hold values from 0 to 255, as said below
- bucket_offsets: int32 [1024], replicated, may hold values from 0 to 1023, as said below
- writer_rank: int32 [1024], replicated, may hold values from 0 to 3, as said below
Outputs:
- saved: bfloat16 [3, 8, 1024, 3584], P(None, 'ep', 'dp')
The draws below stay inside these ranges and needn't reach their ends.
Inputs may be any that keep to these rules, and one draw needn't show every extreme that they name: `expert_ids`: 8 different global expert numbers. `bucket_offsets`: each saved row named exactly once. `writer_rank`: of the bucket rows held by any one dp index, exactly 1024 // (4 * 4) are written by each dp index.
All inputs are finite; a program needn't handle non-finite values.
Results may differ from the reference program's by a relative error of at most 0.001.
Values may be sent and summed in bfloat16 or wider, within the bound.
A program may use at most 128 MiB of HBM per device.

```python
import math
import jax
import jax.numpy as jnp

ROWS = 1024
COLS = 3584
ALL_EXPERTS = 256
EXPERTS = 8
N_DP = 4


def layout_tables(key):
    shard_rows = ROWS // N_DP
    shuffle = jax.random.permutation(jax.random.fold_in(key, 11), ROWS).astype(jnp.int32)
    pattern = jnp.tile(jnp.arange(N_DP, dtype=jnp.int32), shard_rows // N_DP)
    shard_keys = jax.random.split(jax.random.fold_in(key, 12), N_DP)
    chosen = jax.vmap(lambda single: jax.random.permutation(single, pattern))(shard_keys).reshape(ROWS)
    writers = jnp.zeros((ROWS,), jnp.int32).at[shuffle].set(chosen.astype(jnp.int32))
    return (shuffle, writers)


def draw_expert_ids(key, part):
    return jax.random.permutation(jax.random.fold_in(key, 5), ALL_EXPERTS)[:EXPERTS].astype(jnp.int32)


def draw_bucket_offsets(key, part):
    return layout_tables(key)[0]


def draw_writer_rank(key, part):
    return layout_tables(key)[1]


def level_of(key, dims, cuts, least, high):
    level = 1.0
    for dim, parts in cuts:
        draws = jax.random.uniform(jax.random.fold_in(jax.random.fold_in(key, 6), dim), (parts,), jnp.float32, least / len(cuts), high / len(cuts))
        level = level * jnp.repeat(jnp.exp(draws), dims[dim] // parts).reshape((-1,) + (1,) * (len(dims) - 1 - dim))
    return level


def scatter_about(own_key, dims, spread, limit, shards=(), kind=jnp.bfloat16):
    drawn = spread * jax.random.normal(own_key, dims, jnp.float32)
    if shards:
        drawn = drawn * level_of(own_key, dims, shards, -0.22, 0.18)
    return jnp.clip(drawn, -limit, limit).astype(kind)


def setup_inputs(seed: int = 0) -> dict:
    streams_of = jax.random.split(jax.random.key(seed), 7)
    master_weights = scatter_about(streams_of[0], (EXPERTS, ROWS, COLS), 1.0, 6.0, ((0, 8), (1, 4)), jnp.float32)
    first_moment = scatter_about(streams_of[1], (EXPERTS, ROWS, COLS), 1.0, 6.0, ((0, 8), (1, 4)), jnp.float32)
    second_moment = jnp.clip(jnp.exp(math.log(4.0) - 5.9914646 * jax.random.uniform(streams_of[2], (EXPERTS, ROWS, COLS), jnp.float32) ** level_of(streams_of[2], (EXPERTS, ROWS, COLS), ((0, 8), (1, 4)), -0.2, 0.2)), 0.01, 4.0)
    expert_ids = draw_expert_ids(jax.random.fold_in(streams_of[6], 71), 0)
    bucket_offsets = draw_bucket_offsets(jax.random.fold_in(streams_of[6], 71), 0)
    writer_rank = draw_writer_rank(jax.random.fold_in(streams_of[6], 71), 0)
    return {"master_weights": master_weights, "first_moment": first_moment, "second_moment": second_moment, "expert_ids": expert_ids, "bucket_offsets": bucket_offsets, "writer_rank": writer_rank}


def destinations(bucket_offsets, writer_rank, shard_rows, groups):
    indicator = (writer_rank[:, None] == jnp.arange(groups, dtype=jnp.int32)[None, :]).astype(jnp.int32)
    before = jnp.cumsum(indicator, axis=0) - indicator
    within = jnp.sum(before * indicator, axis=1).astype(jnp.int32)
    placed = writer_rank * shard_rows + within
    return jnp.take(placed, bucket_offsets)


def reference(master_weights, first_moment, second_moment, expert_ids, bucket_offsets, writer_rank):
    target = destinations(bucket_offsets, writer_rank, ROWS // N_DP, N_DP)
    source_rows = jnp.argsort(target)
    source_order = jnp.argsort(expert_ids)

    def arrange(field):
        moved = jnp.take(field.astype(jnp.bfloat16), source_order, axis=0)
        return jnp.take(moved, source_rows, axis=1)

    return jnp.stack([arrange(master_weights), arrange(first_moment), arrange(second_moment)])
```

```python
import functools
import math

import jax
import jax.numpy as jnp
from jax import lax
from jax.experimental import pallas as pl
from jax.experimental.pallas import tpu as pltpu
from jax.sharding import PartitionSpec as P

MESH = pl.DeviceIdType.MESH
FIELDS = 3


def tables(bucket_offsets, writer_rank, mine, groups):
    total = bucket_offsets.shape[0]
    shard = total // groups
    pair = shard // groups
    p = jnp.arange(total, dtype=jnp.int32)
    q = jnp.arange(shard, dtype=jnp.int32)
    earlier = (writer_rank[None, :] == writer_rank[:, None]) & (p[None, :] < p[:, None])
    place = writer_rank * shard + jnp.sum(earlier.astype(jnp.int32), axis=1)
    target = jnp.sum(jnp.where(bucket_offsets[:, None] == p[None, :], place[None, :], 0), axis=1)
    dest = (target // shard).reshape(groups, shard)
    ahead = (dest[:, None, :] == dest[:, :, None]) & (q[None, None, :] < q[None, :, None])
    rank = jnp.sum(ahead.astype(jnp.int32), axis=2)
    position = lax.dynamic_index_in_dim(dest * pair + rank, mine, 0, keepdims=False)
    before = (position[None, :] == q[:, None]).astype(jnp.bfloat16)
    arrives = (jnp.arange(groups, dtype=jnp.int32)[:, None] * pair + rank).reshape(total)
    slot = (target[None, :] == (mine * shard + q)[:, None]).astype(jnp.bfloat16)
    entry = (arrives[None, :] == q[:, None]).astype(jnp.bfloat16)
    after = lax.dot_general(
        slot, entry, (((1,), (1,)), ((), ())), preferred_element_type=jnp.float32
    ).astype(jnp.bfloat16)
    return before, after


def order_of(expert_ids):
    count = expert_ids.shape[0]
    k = jnp.arange(count, dtype=jnp.int32)
    rank = jnp.sum((expert_ids[None, :] < expert_ids[:, None]).astype(jnp.int32), axis=1)
    return jnp.sum(jnp.where(rank[None, :] == k[:, None], k[None, :], 0), axis=1)


def sort_kernel(order_ref, a_ref, b_ref, c_ref, out_ref):
    for f, ref in enumerate((a_ref, b_ref, c_ref)):
        out_ref[f] = jnp.dot(
            order_ref[...], ref[...].astype(jnp.bfloat16), preferred_element_type=jnp.float32
        ).astype(jnp.bfloat16)


def place_kernel(order_ref, rows_ref, out_ref):
    for f in range(FIELDS):
        out_ref[f] = jnp.dot(
            order_ref[...], rows_ref[f], preferred_element_type=jnp.float32
        ).astype(jnp.bfloat16)


def tile_of(cols):
    return next(t for t in (512, 256, 128, cols) if cols % t == 0)


def sort_rows(order, a, b, c):
    rows, cols = a.shape
    tile = tile_of(cols)
    block = pl.BlockSpec((rows, tile), lambda i: (0, i))
    return pl.pallas_call(
        sort_kernel,
        grid=(cols // tile,),
        in_specs=[pl.BlockSpec((rows, rows), lambda i: (0, 0)), block, block, block],
        out_specs=pl.BlockSpec((FIELDS, rows, tile), lambda i: (0, 0, i)),
        out_shape=jax.ShapeDtypeStruct((FIELDS, rows, cols), jnp.bfloat16),
    )(order, a, b, c)


def place_rows(order, arrived):
    fields, rows, cols = arrived.shape
    tile = tile_of(cols)
    block = pl.BlockSpec((fields, rows, tile), lambda i: (0, 0, i))
    return pl.pallas_call(
        place_kernel,
        grid=(cols // tile,),
        in_specs=[pl.BlockSpec((rows, rows), lambda i: (0, 0)), block],
        out_specs=block,
        out_shape=jax.ShapeDtypeStruct(arrived.shape, jnp.bfloat16),
    )(order, arrived)


def partner(me, offset, n):
    out, bit = 0, 1
    while bit < n:
        out = out + ((me // bit + (offset // bit) % 2) % 2) * bit
        bit *= 2
    return out


def exchange_kernel(n_ep, n_dp, half, order_ref, s_ref, out_ref, *scratch):
    e1 = scratch[: 2 * FIELDS]
    sel, mid, sems = scratch[2 * FIELDS], scratch[2 * FIELDS + 1], scratch[2 * FIELDS + 2 :]
    z_send, z_recv, a_send, a_recv, b_send, b_recv = sems
    ep, dp = lax.axis_index("ep"), lax.axis_index("dp")
    blocks = s_ref.shape[1]
    m_ep, m_dp = blocks // n_ep, blocks // n_dp
    z_order = sorted(range(1, n_dp), key=lambda o: -o)
    e_order = sorted(range(1, n_ep), key=lambda o: (o == 1, o % 2, -o))
    first = pl.ds(0, half)
    last = pl.ds(half, s_ref.shape[3] - half)

    barrier = pltpu.get_barrier_semaphore()
    for o in range(1, n_dp):
        pl.semaphore_signal(barrier, inc=1, device_id={"dp": partner(dp, o, n_dp)}, device_id_type=MESH)
    for o in range(1, n_ep):
        pl.semaphore_signal(barrier, inc=1, device_id={"ep": partner(ep, o, n_ep)}, device_id_type=MESH)
    pl.semaphore_wait(barrier, n_dp + n_ep - 2)

    def remote(src, dst, send, recv, axis, peer):
        return pltpu.make_async_remote_copy(
            src_ref=src, dst_ref=dst, send_sem=send, recv_sem=recv,
            device_id={axis: peer}, device_id_type=MESH,
        )

    def refs(c):
        f = c % FIELDS
        if c < FIELDS:
            return s_ref.at[f, :, :, first], mid.at[c], mid.at[c], out_ref.at[f, :, :, first]
        whole = s_ref.at[f, :, :, last]
        return mid.at[c], out_ref.at[f, :, :, last], whole, mid.at[c]

    def z_copies(c):
        src, dst, _, _ = refs(c)
        return [
            remote(
                src.at[pl.ds(partner(dp, o, n_dp) * m_dp, m_dp)], dst.at[pl.ds(dp * m_dp, m_dp)],
                z_send.at[c, o], z_recv.at[c, o], "dp", partner(dp, o, n_dp),
            )
            for o in z_order
        ]

    def a_copies(c):
        src = refs(c)[2]
        return [
            remote(
                src.at[pl.ds(partner(ep, o, n_ep) * m_ep, m_ep)], e1[c].at[ep],
                a_send.at[c, o], a_recv.at[c, o], "ep", partner(ep, o, n_ep),
            )
            for o in e_order
        ]

    def b_copies(c):
        dst = refs(c)[3]
        return [
            remote(
                sel.at[c, partner(ep, o, n_ep)], dst.at[pl.ds(ep * m_ep, m_ep)],
                b_send.at[c, o], b_recv.at[c, o], "ep", partner(ep, o, n_ep),
            )
            for o in e_order
        ]

    def start(copies):
        for copy in copies:
            copy.start()

    def arrive(copies):
        for copy in copies:
            copy.wait_recv()

    def z_start(c):
        start(z_copies(c))
        src, dst, _, _ = refs(c)
        own = pl.ds(dp * m_dp, m_dp)
        dst[own] = src[own]

    def a_start(c):
        start(a_copies(c))
        e1[c][ep] = refs(c)[2][pl.ds(ep * m_ep, m_ep)]

    def a_to_b(c):
        arrive(a_copies(c))
        for k in range(n_ep):
            sel[c, k] = e1[c][order_ref[k]]
        start(b_copies(c))
        refs(c)[3][pl.ds(ep * m_ep, m_ep)] = sel[c, ep]

    def z_to_a(c):
        arrive(z_copies(c))
        a_start(c)

    def b_to_z(c):
        arrive(b_copies(c))
        z_start(c)

    for f in range(FIELDS):
        a_start(FIELDS + f)
        z_start(f)
    a_to_b(3)
    a_to_b(4)
    z_to_a(0)
    a_to_b(5)
    b_to_z(3)
    z_to_a(1)
    b_to_z(4)
    a_to_b(0)
    b_to_z(5)
    z_to_a(2)
    a_to_b(1)
    a_to_b(2)
    for c in range(FIELDS):
        arrive(z_copies(FIELDS + c))
        arrive(b_copies(c))
    for c in range(2 * FIELDS):
        for copies in (z_copies(c), a_copies(c), b_copies(c)):
            for copy in copies:
                copy.wait_send()


def exchange(order, stacked, n_ep, n_dp):
    fields, blocks, depth, cols = stacked.shape
    half = cols // 256 * 128
    per = blocks // n_ep
    dma = pltpu.SemaphoreType.DMA
    return pl.pallas_call(
        functools.partial(exchange_kernel, n_ep, n_dp, half),
        out_shape=jax.ShapeDtypeStruct(stacked.shape, stacked.dtype),
        in_specs=[
            pl.BlockSpec(memory_space=pltpu.SMEM),
            pl.BlockSpec(memory_space=pltpu.VMEM),
        ],
        out_specs=pl.BlockSpec(memory_space=pltpu.VMEM),
        scratch_shapes=[pltpu.VMEM((n_ep, per, depth, half), stacked.dtype)] * (2 * fields)
        + [
            pltpu.VMEM((2 * fields, n_ep, per, depth, half), stacked.dtype),
            pltpu.VMEM((2 * fields, blocks, depth, half), stacked.dtype),
            dma((2 * fields, n_dp)),
            dma((2 * fields, n_dp)),
            dma((2 * fields, n_ep)),
            dma((2 * fields, n_ep)),
            dma((2 * fields, n_ep)),
            dma((2 * fields, n_ep)),
        ],
        compiler_params=pltpu.CompilerParams(collective_id=0, has_side_effects=True),
    )(order, stacked)


def on_device(master_weights, first_moment, second_moment, expert_ids, bucket_offsets, writer_rank):
    n_dp, n_ep = lax.axis_size("dp"), lax.axis_size("ep")
    _, rows, cols = master_weights.shape
    before, after = tables(bucket_offsets, writer_rank, lax.axis_index("dp"), n_dp)
    stacked = sort_rows(before, master_weights[0], first_moment[0], second_moment[0])
    depth = math.gcd(rows // n_dp, rows // n_ep)
    arrived = exchange(
        order_of(expert_ids), stacked.reshape(FIELDS, rows // depth, depth, cols), n_ep, n_dp
    )
    return place_rows(after, arrived.reshape(FIELDS, rows, cols))[:, None]


def solution(mesh):
    return jax.shard_map(
        on_device,
        mesh=mesh,
        in_specs=(P("ep", "dp", None), P("ep", "dp", None), P("ep", "dp", None), P(), P(), P()),
        out_specs=P(None, "ep", "dp", None),
        check_vma=False,
    )
```
